128 devices in a mesh: gx: 16 (over y, z), gy: 8 (over x, core).
Axes of the slice: x: 4, y: 4, z: 4, core: 2. Of those that a mesh axis runs over, the one named last changes fastest.
Arguments:
- states: bfloat16 [80, 8, 512, 2048], P('gx', None, 'gy'), may hold values from -6 to 6
- obs_pert: bfloat16 [80, 8, 2048], P(None, 'gy', 'gx'), may hold values from -6 to 6
- obs_innov: bfloat16 [8, 2048], P('gy', 'gx'), may hold values from -6 to 6
- obs_cell: int32 [8, 2048], P('gy', 'gx'), may hold values from 0 to 8191
- obs_count: int32 [8, 16], P('gy', 'gx'), may hold values from 16 to 128, as said below
Outputs:
- analysis: bfloat16 [80, 8, 512, 2048], P(None, None, 'gy', 'gx')
The draws below stay inside these ranges and needn't reach their ends.
Inputs may be any that keep to these rules, and one draw needn't show every extreme that they name: `obs_count`: at most 128; some tile has exactly 128. `obs_cell`: slots at or after their tile's count are unused.
All inputs are finite; a program needn't handle non-finite values.
Results may differ from the reference program's by a relative error of at most 0.0057.
Values may be sent and summed in bfloat16 or wider, within the bound.
A program may use at most 128 MiB of HBM per device.

```python
import jax
import jax.numpy as jnp
from jax import lax

K = 80
L = 8
TX = 128
TY = 64
OBS_DEV = 128
NS_ITERS = 4
NX = 2048
NY = 512
TILE_ROWS = 8
TILE_COLS = 16
OBS_COLS = 2048


def draw_obs_count(key, part):
    base = jax.random.randint(key, (TILE_ROWS * TILE_COLS,), OBS_DEV // 8, OBS_DEV + 1)
    spot = jax.random.randint(jax.random.fold_in(key, 7), (), 0, TILE_ROWS * TILE_COLS)
    flat = jnp.where(jnp.arange(TILE_ROWS * TILE_COLS) == spot, OBS_DEV, base)
    return flat.reshape(TILE_ROWS, TILE_COLS).astype(jnp.int32)


def plant(entries, own_key, least, top_value):
    extent = entries.shape
    index_at = [jax.random.randint(jax.random.fold_in(own_key, axis), (), 0, extent[axis]) for axis in range(len(extent))]
    entries = entries.at[tuple(index_at)].set(least)
    longest = extent.index(max(extent))
    index_at[longest] = (index_at[longest] + 1) % extent[longest]
    return entries.at[tuple(index_at)].set(top_value)


def block_levels(rng, extent, split, least, top_value):
    def one(axis_at, parts):
        draws = jax.random.uniform(jax.random.fold_in(jax.random.fold_in(rng, 6), axis_at), (parts,), jnp.float32, least / len(split), top_value / len(split))
        return jnp.repeat(jnp.exp(draws), extent[axis_at] // parts).reshape((-1,) + (1,) * (len(extent) - axis_at - 1))

    factor_of = one(*split[0])
    for cut in split[1:]:
        factor_of = factor_of * one(*cut)
    return factor_of


def noise(rng, extent, scale, most, cuts=(), kind=jnp.bfloat16):
    values = scale * jax.random.normal(rng, extent, jnp.float32)
    if cuts:
        values = values * block_levels(rng, extent, cuts, -0.22, 0.18)
    return jnp.clip(values, -most, most).astype(kind)


def setup_inputs(seed: int = 0) -> dict:
    streams_of = jax.random.split(jax.random.key(seed), 6)
    return {
        "states": noise(streams_of[0], (K, L, NY, NX), 1.0, 6.0, ((0, 16), (2, 8))),
        "obs_pert": noise(streams_of[1], (K, TILE_ROWS, OBS_COLS), 1.0, 6.0, ((1, 8), (2, 16))),
        "obs_innov": noise(streams_of[2], (TILE_ROWS, OBS_COLS), 1.0, 6.0, ((0, 8), (1, 16))),
        "obs_cell": plant(jax.random.randint(streams_of[3], (TILE_ROWS, OBS_COLS), 0, TY * TX), jax.random.fold_in(streams_of[3], 1), 0, (TY * TX) - 1).astype(jnp.int32),
        "obs_count": draw_obs_count(jax.random.fold_in(streams_of[5], 71), 0),
    }


def locality(groups, row_index, col_index, tile_rows, tile_cols):
    slot_count = groups.shape[1] // 9
    width_x = TX * tile_cols
    height_y = TY * tile_rows
    position = lax.broadcasted_iota(jnp.int32, (1, 9 * slot_count), 1)
    row_shift = position // (3 * slot_count) - 1
    col_shift = position // slot_count % 3 - 1
    folded = jnp.logical_and(row_index == tile_rows - 1, row_shift == 1)
    src_row = jnp.where(folded, tile_rows - 1, row_index + row_shift)
    src_col = jnp.where(folded, (tile_cols - 1 - col_index + col_shift) % tile_cols, (col_index + col_shift) % tile_cols)
    local_row = groups[-2:-1].astype(jnp.float32)
    local_col = groups[-1:].astype(jnp.float32)
    obs_y = src_row.astype(jnp.float32) * TY + local_row
    obs_x = src_col.astype(jnp.float32) * TX + local_col
    obs_y = jnp.where(folded, 2.0 * height_y - 1.0 - obs_y, obs_y)
    obs_x = jnp.where(folded, width_x - 1.0 - obs_x, obs_x)
    block_y = (row_index * TY + lax.broadcasted_iota(jnp.int32, (TY, 1), 0)).astype(jnp.float32)
    gap_y = obs_y - block_y
    offset = jnp.mod(obs_x - (col_index * TX).astype(jnp.float32), float(width_x))
    gap_x = jnp.where(offset < TX, 0.0, jnp.minimum(offset - (TX - 1.0), width_x - offset))
    radius = float(TY // 2)
    scaled = jnp.minimum(1.0, (gap_x * gap_x + gap_y * gap_y) / (radius * radius))
    return (1.0 - scaled) * (1.0 - scaled)

def batched(left, right):
    return jnp.einsum('bij,bjk->bik', left, right, precision=lax.Precision.HIGHEST)

def transforms(groups, taper, members):
    rows = groups[:members + 1]
    weighted = (rows.astype(jnp.float32)[None] * taper[:, None, :]).astype(jnp.bfloat16)
    products = jnp.einsum('bks,js->bkj', weighted.astype(jnp.float32), groups[:members].astype(jnp.float32))
    covariance = products[:, :members, :]
    projected = products[:, members, :]
    identity = jnp.eye(members, dtype=jnp.float32)
    system = identity[None] + covariance / (members - 1.0)
    norm_scale = jnp.sqrt(lax.optimization_barrier(jnp.sum(system * system, axis=(1, 2))))[:, None, None]
    iterate = system / norm_scale
    inverse = jnp.broadcast_to(identity, system.shape)
    for sweep in range(NS_ITERS):
        correction = 1.5 * identity[None] - 0.5 * batched(inverse, iterate)
        iterate = batched(iterate, correction)
        inverse = batched(correction, inverse)
    spread_weights = inverse / jnp.sqrt(norm_scale)
    mean_weights = batched(inverse, batched(inverse, projected[:, :, None])) / (norm_scale * (members - 1.0))
    return (spread_weights + mean_weights).astype(jnp.bfloat16)

def analysis_step(tile_states, transform):
    average = lax.optimization_barrier(jnp.mean(tile_states.astype(jnp.float32), axis=0))
    perturb = (tile_states.astype(jnp.float32) - average[None]).astype(jnp.bfloat16)
    mixed_members = jnp.einsum('klrx,rkj->jlrx', perturb.astype(jnp.float32), transform.astype(jnp.float32))
    return (average[None] + mixed_members).astype(jnp.bfloat16)

def reference(states, obs_pert, obs_innov, obs_cell, obs_count):
    tile_rows = TILE_ROWS
    tile_cols = TILE_COLS
    members = K
    filled = jnp.arange(OBS_DEV, dtype=jnp.int32)[None, None, :] < obs_count[:, :, None]
    perturbs = obs_pert.reshape(members, tile_rows, tile_cols, OBS_DEV)
    perturbs = jnp.where(filled[None], perturbs, jnp.zeros_like(perturbs))
    innovation = obs_innov.reshape(tile_rows, tile_cols, OBS_DEV)
    innovation = jnp.where(filled, innovation, jnp.zeros_like(innovation))
    obs_cells = obs_cell.reshape(tile_rows, tile_cols, OBS_DEV)
    packed = jnp.concatenate([perturbs, innovation[None], (obs_cells // TX).astype(jnp.bfloat16)[None], (obs_cells % TX).astype(jnp.bfloat16)[None]], axis=0)

    def one_tile(tile_index):
        row_index = tile_index // tile_cols
        col_index = tile_index % tile_cols
        pieces = []
        for row_shift in (-1, 0, 1):
            for col_shift in (-1, 0, 1):
                present = jnp.bool_(True)
                if row_shift == 1:
                    folded = row_index == tile_rows - 1
                    src_row = jnp.where(folded, tile_rows - 1, row_index + 1)
                    src_col = jnp.where(folded, (tile_cols - 1 - col_index + col_shift) % tile_cols, (col_index + col_shift) % tile_cols)
                elif row_shift == -1:
                    src_row = jnp.maximum(row_index - 1, 0)
                    src_col = (col_index + col_shift) % tile_cols
                    present = row_index > 0
                else:
                    src_row = row_index
                    src_col = (col_index + col_shift) % tile_cols
                neighbour = packed[:, src_row.astype(jnp.int32), src_col.astype(jnp.int32), :]
                pieces.append(jnp.where(present, neighbour, jnp.zeros_like(neighbour)))
        groups = jnp.concatenate(pieces, axis=1)
        taper = locality(groups, row_index, col_index, tile_rows, tile_cols)
        transform = transforms(groups, taper, members)
        tile_states = lax.dynamic_slice(states, (jnp.int32(0), jnp.int32(0), (row_index * TY).astype(jnp.int32), (col_index * TX).astype(jnp.int32)), (members, L, TY, TX))
        return analysis_step(tile_states, transform)
    tiles = lax.map(one_tile, jnp.arange(tile_rows * tile_cols, dtype=jnp.int32))
    tiles = tiles.reshape(tile_rows, tile_cols, members, L, TY, TX)
    return tiles.transpose(2, 3, 0, 4, 1, 5).reshape(members, L, TY * tile_rows, TX * tile_cols)
```

```python
import functools

import jax
import jax.numpy as jnp
from jax import lax
from jax.experimental import pallas as pl
from jax.experimental.pallas import tpu as pltpu
from jax.sharding import PartitionSpec as P

MESH = pl.DeviceIdType.MESH
F32 = jnp.float32
BF16 = jnp.bfloat16

TX = 128
TY = 64
NS_ITERS = 4
RB = 8
PK = 96
LANES = 128


def wrap(value, count):
    return lax.rem(value + count, count)


def split(value):
    high = value.astype(BF16)
    low = (value - high.astype(F32)).astype(BF16)
    return high, low


def tall(value):
    rows = value.shape[0]
    return jnp.concatenate([value, jnp.zeros((LANES - rows, value.shape[1]), value.dtype)], axis=0)


def product(left, right):
    lh, ll = left
    rh, rl = (tall(part) for part in right)
    lhs = jnp.concatenate([lh, ll], axis=1)
    rhs = jnp.concatenate(
        [
            jnp.concatenate([rh, rl], axis=1),
            jnp.concatenate([rh, jnp.zeros_like(rl)], axis=1),
        ],
        axis=0,
    )
    both = jnp.dot(lhs, rhs, preferred_element_type=F32)
    return both[:, :LANES] + both[:, LANES:]


def kernel(
    members,
    levels,
    nrows,
    ncols,
    states,
    packed,
    out,
    fields,
    groups,
    right,
    weighted,
    products,
    tmat,
    spread,
    mixed,
    own_sem,
    state_send,
    state_recv,
    obs_send,
    obs_recv,
):
    col = lax.axis_index("gx")
    row = lax.axis_index("gy")
    share = members // ncols
    chunks = TY // RB

    barrier = pltpu.get_barrier_semaphore()

    def greet(coords):
        pl.semaphore_signal(barrier, inc=1, device_id=coords, device_id_type=MESH)

    for d in range(1, ncols):
        greet({"gx": lax.rem(col + d, ncols)})
    for a in (-1, 1):

        @pl.when(jnp.logical_and(row + a >= 0, row + a < nrows))
        def _():
            for b in (-1, 0, 1):
                greet({"gx": wrap(col + b, ncols), "gy": row + a})

    inner = jnp.logical_and(row > 0, row < nrows - 1)
    pl.semaphore_wait(barrier, ncols - 1 + jnp.where(inner, 6, 3))

    def obs_copy(slot, a, coords):
        return pltpu.make_async_remote_copy(
            src_ref=packed,
            dst_ref=groups.at[slot],
            send_sem=obs_send.at[slot],
            recv_sem=obs_recv.at[a + 1],
            device_id=coords,
            device_id_type=MESH,
        )

    def obs_plain(a, b, act):
        slot = (a + 1) * 3 + b + 1
        if a == 0 and b == 0:
            return

        def go():
            act(obs_copy(slot, a, {"gx": wrap(col - b, ncols), "gy": row - a}))

        if a == 0:
            go()
        else:
            pl.when(jnp.logical_and(row - a >= 0, row - a < nrows))(go)

    def obs_fold(b, act, act_local):
        slot = 6 + b + 1
        target = lax.rem(2 * ncols - 1 + b - col, ncols)
        at_fold = row == nrows - 1

        @pl.when(jnp.logical_and(at_fold, target != col))
        def _():
            act(
                pltpu.make_async_remote_copy(
                    src_ref=packed,
                    dst_ref=groups.at[slot],
                    send_sem=obs_send.at[9 + b + 1],
                    recv_sem=obs_recv.at[2],
                    device_id={"gx": target},
                    device_id_type=MESH,
                )
            )

        if act_local:

            @pl.when(jnp.logical_and(at_fold, target == col))
            def _():
                pltpu.make_async_copy(packed, groups.at[slot], obs_recv.at[2]).start()

    for a in (0, 1, -1):
        for b in (-1, 0, 1):
            obs_plain(a, b, lambda copy: copy.start())
    for b in (-1, 0, 1):
        obs_fold(b, lambda copy: copy.start(), True)
    pltpu.make_async_copy(packed, groups.at[4], obs_recv.at[1]).start()

    side = 4

    def distance(d):
        dy, dz = d // side, d % side
        return min(dy, side - dy) + min(dz, side - dz)

    order = sorted(range(1, ncols), key=distance)
    yy = col // side
    zz = lax.rem(col, side)

    def states_of(target, c):
        return states.at[
            :, :, pl.ds(pl.multiple_of(c * RB, RB), RB), pl.ds(pl.multiple_of(target * TX, TX), TX)
        ]

    def issue(c, _):
        pltpu.make_async_copy(
            states_of(col, c), fields.at[c, pl.ds(col * share, share)], state_recv.at[c]
        ).start()
        for d in order:
            target = lax.rem(yy + d // side, side) * side + lax.rem(zz + d % side, side)
            pltpu.make_async_remote_copy(
                src_ref=states_of(target, c),
                dst_ref=fields.at[c, pl.ds(col * share, share)],
                send_sem=state_send.at[c],
                recv_sem=state_recv.at[c],
                device_id={"gx": target},
                device_id_type=MESH,
            ).start()
        return 0

    lax.fori_loop(0, chunks, issue, 0)

    @pl.when(row == 0)
    def _():
        groups[0:3] = jnp.zeros((3, PK, LANES), BF16)

    @pl.when(row > 0)
    def _():
        three = groups.at[0:3]
        pltpu.make_async_copy(three, three, obs_recv.at[0]).wait()

    for a in (0, 1):
        three = groups.at[3 * (a + 1) : 3 * (a + 2)]
        pltpu.make_async_copy(three, three, obs_recv.at[a + 1]).wait()

    live = lax.broadcasted_iota(jnp.int32, (LANES, LANES), 0) < members
    for g in range(9):
        part = jnp.concatenate([groups[g], jnp.zeros((LANES - PK, LANES), BF16)], axis=0)
        right[:, g * LANES : (g + 1) * LANES] = jnp.where(
            live, part.astype(F32), 0.0
        ).astype(BF16)

    eye = (
        lax.broadcasted_iota(jnp.int32, (members, LANES), 0)
        == lax.broadcasted_iota(jnp.int32, (members, LANES), 1)
    ).astype(F32)
    width_x = float(TX * ncols)
    height_y = float(TY * nrows)

    def weigh(c):
        block_y = (
            row * TY + c * RB + lax.broadcasted_iota(jnp.int32, (RB, LANES), 0)
        ).astype(F32)
        for g in range(9):
            a, b = g // 3 - 1, g % 3 - 1
            around = groups[g].astype(F32)
            src_row = row + a
            src_col = wrap(col + b, ncols)
            local_row = around[members + 1 : members + 2]
            local_col = around[members + 2 : members + 3]
            if a == 1:
                folded = row == nrows - 1
                src_row = jnp.where(folded, nrows - 1, src_row)
                src_col = jnp.where(folded, wrap(ncols - 1 - col + b, ncols), src_col)
            obs_y = (src_row * TY).astype(F32) + local_row
            obs_x = (src_col * TX).astype(F32) + local_col
            if a == 1:
                turn = jnp.where(folded, 1.0, 0.0)
                obs_y = obs_y + turn * (2.0 * height_y - 1.0 - 2.0 * obs_y)
                obs_x = obs_x + turn * (width_x - 1.0 - 2.0 * obs_x)
            gap_y = obs_y - block_y
            offset = obs_x - (col * TX).astype(F32)
            offset = jnp.where(offset < 0.0, offset + width_x, offset)
            gap_x = jnp.where(
                offset < TX, 0.0, jnp.minimum(offset - (TX - 1.0), width_x - offset)
            )
            radius = float(TY // 2)
            scaled = jnp.minimum(1.0, (gap_x * gap_x + gap_y * gap_y) / (radius * radius))
            taper = (1.0 - scaled) * (1.0 - scaled)
            for r in range(RB):
                weighted[r * PK : (r + 1) * PK, g * LANES : (g + 1) * LANES] = (
                    around * taper[r : r + 1]
                ).astype(BF16)
        products[...] = lax.dot_general(
            weighted[...],
            right[...],
            (((1,), (1,)), ((), ())),
            preferred_element_type=F32,
        )

    def transforms(rows):
        scale, iterate, inverse = {}, {}, {}
        for r in rows:
            cov = products[r * PK : r * PK + members]
            system = eye + tall(cov).T[:members] * (1.0 / (members - 1.0))
            total = jnp.sum(jnp.sum(system * system, axis=0, keepdims=True), axis=1, keepdims=True)
            scale[r] = jnp.sqrt(total)
            iterate[r] = system / scale[r]
        for r in rows:
            inverse[r] = 1.5 * eye - 0.5 * iterate[r]
        iterate = {r: product(split(iterate[r]), split(inverse[r])) for r in rows}
        for sweep in range(1, NS_ITERS):
            inv = {r: split(inverse[r]) for r in rows}
            itr = {r: split(iterate[r]) for r in rows}
            both = {r: product(inv[r], itr[r]) for r in rows}
            cor = {r: split(1.5 * eye - 0.5 * both[r]) for r in rows}
            if sweep < NS_ITERS - 1:
                iterate = {r: product(itr[r], cor[r]) for r in rows}
            inverse = {r: product(cor[r], inv[r]) for r in rows}
        for r in rows:
            inv = split(inverse[r])
            projected = products[r * PK + members : r * PK + members + 8]
            once = product(split(projected), inv)
            mean = product(split(once), inv)[0:1]
            tmat[r] = (
                inverse[r] / jnp.sqrt(scale[r]) + mean / (scale[r] * (members - 1.0))
            ).astype(BF16)

    def analyse(c):
        for pair in range(levels // 2):
            averages = []
            for half in range(2):
                lev = 2 * pair + half
                field = fields[c, :, lev].astype(F32)
                average = jnp.sum(field, axis=0) * (1.0 / members)
                averages.append(average)
                spread[half] = (field - average[None]).reshape(members * RB, LANES)
            for r in range(RB):
                perturb = jnp.concatenate(
                    [
                        tall(spread[half, pl.ds(r, members, stride=RB), :].astype(BF16))
                        for half in range(2)
                    ],
                    axis=1,
                )
                mix = jnp.dot(tmat[r], perturb, preferred_element_type=F32)
                for half in range(2):
                    mixed[half, pl.ds(r, members, stride=RB), :] = mix[
                        :, half * LANES : (half + 1) * LANES
                    ]
            for half in range(2):
                lev = 2 * pair + half
                value = mixed[half].reshape(members, RB, LANES) + averages[half][None]
                out[c, :, lev] = value.astype(BF16)

    def step(c, _):
        weigh(c)
        for first in range(0, RB, 4):
            transforms(range(first, first + 4))
        pltpu.make_async_copy(fields.at[c], fields.at[c], state_recv.at[c]).wait()
        analyse(c)
        return 0

    lax.fori_loop(0, chunks, step, 0)

    def sent(c, _):
        part = fields.at[c, 0 : (ncols - 1) * share]
        pltpu.make_async_copy(part, part, state_send.at[c]).wait()
        return 0

    lax.fori_loop(0, chunks, sent, 0)
    for a in (0, 1, -1):
        for b in (-1, 0, 1):
            obs_plain(a, b, lambda copy: copy.wait_send())
    for b in (-1, 0, 1):
        obs_fold(b, lambda copy: copy.wait_send(), False)


def place(chunks, rows, done, out, sem):
    copies = [
        pltpu.make_async_copy(done.at[c], out.at[:, :, c * rows : (c + 1) * rows, :], sem.at[c])
        for c in range(chunks)
    ]
    for copy in copies:
        copy.start()
    for copy in copies:
        copy.wait()


def body(states, obs_pert, obs_innov, obs_cell, obs_count):
    members = obs_pert.shape[0]
    slots = obs_pert.shape[2]
    levels = states.shape[1]
    ncols = lax.axis_size("gx")
    nrows = lax.axis_size("gy")
    filled = lax.broadcasted_iota(jnp.int32, (1, slots), 1) < obs_count
    perturbs = jnp.where(filled, obs_pert[:, 0, :], jnp.zeros((), BF16))
    innovation = jnp.where(filled, obs_innov, jnp.zeros((), BF16))
    packed = jnp.concatenate(
        [
            perturbs,
            innovation,
            (obs_cell // TX).astype(BF16),
            (obs_cell % TX).astype(BF16),
            jnp.zeros((PK - members - 3, slots), BF16),
        ],
        axis=0,
    )
    chunks = TY // RB
    done = pl.pallas_call(
        functools.partial(kernel, members, levels, nrows, ncols),
        out_shape=jax.ShapeDtypeStruct((chunks, members, levels, RB, TX), BF16),
        in_specs=[pl.BlockSpec(memory_space=pl.ANY), pl.BlockSpec(memory_space=pl.ANY)],
        out_specs=pl.BlockSpec(memory_space=pltpu.VMEM),
        scratch_shapes=[
            pltpu.VMEM((chunks, members, levels, RB, TX), BF16),
            pltpu.VMEM((9, PK, LANES), BF16),
            pltpu.VMEM((LANES, 9 * LANES), BF16),
            pltpu.VMEM((RB * PK, 9 * LANES), BF16),
            pltpu.VMEM((RB * PK, LANES), F32),
            pltpu.VMEM((RB, members, LANES), BF16),
            pltpu.VMEM((2, members * RB, LANES), F32),
            pltpu.VMEM((2, members * RB, LANES), F32),
            pltpu.SemaphoreType.DMA,
            pltpu.SemaphoreType.DMA((chunks,)),
            pltpu.SemaphoreType.DMA((chunks,)),
            pltpu.SemaphoreType.DMA((12,)),
            pltpu.SemaphoreType.DMA((3,)),
        ],
        compiler_params=pltpu.CompilerParams(
            collective_id=0, has_side_effects=True, vmem_limit_bytes=40 << 20
        ),
        name="exchange",
    )(states, packed)
    return pl.pallas_call(
        functools.partial(place, chunks, RB),
        out_shape=jax.ShapeDtypeStruct((members, levels, TY, TX), BF16),
        in_specs=[pl.BlockSpec(memory_space=pltpu.VMEM)],
        out_specs=pl.BlockSpec(memory_space=pl.ANY),
        scratch_shapes=[pltpu.SemaphoreType.DMA((chunks,))],
        compiler_params=pltpu.CompilerParams(vmem_limit_bytes=16 << 20),
        name="place",
    )(done)


def solution(mesh):
    return jax.shard_map(
        body,
        mesh=mesh,
        in_specs=(
            P("gx", None, "gy", None),
            P(None, "gy", "gx"),
            P("gy", "gx"),
            P("gy", "gx"),
            P("gy", "gx"),
        ),
        out_specs=P(None, None, "gy", "gx"),
        check_vma=False,
    )
```

```python
import functools

import jax
import jax.numpy as jnp
from jax import lax
from jax.experimental import pallas as pl
from jax.experimental.pallas import tpu as pltpu
from jax.sharding import PartitionSpec as P

MESH = pl.DeviceIdType.MESH
F32 = jnp.float32
BF16 = jnp.bfloat16

TX = 128
TY = 64
NS_ITERS = 4
RB = 8
PK = 96
LANES = 128


def wrap(value, count):
    return lax.rem(value + count, count)


def split(value):
    high = value.astype(BF16)
    low = (value - high.astype(F32)).astype(BF16)
    return high, low


def tall(value):
    rows = value.shape[0]
    return jnp.concatenate([value, jnp.zeros((LANES - rows, value.shape[1]), value.dtype)], axis=0)


def product(left, right):
    lh, ll = left
    rh, rl = (tall(part) for part in right)
    lhs = jnp.concatenate([lh, ll], axis=1)
    rhs = jnp.concatenate(
        [
            jnp.concatenate([rh, rl], axis=1),
            jnp.concatenate([rh, jnp.zeros_like(rl)], axis=1),
        ],
        axis=0,
    )
    both = jnp.dot(lhs, rhs, preferred_element_type=F32)
    return both[:, :LANES] + both[:, LANES:]


def analyse(members, fields, tmat, spread, mixed, results, pair):
    averages = []
    for half in range(2):
        field = fields[:, 2 * pair + half].astype(F32)
        average = jnp.sum(field, axis=0) * (1.0 / members)
        averages.append(average)
        spread[half] = (field - average[None]).reshape(members * RB, LANES)
    for r in range(RB):
        perturb = jnp.concatenate(
            [
                tall(spread[half, pl.ds(r, members, stride=RB), :].astype(BF16))
                for half in range(2)
            ],
            axis=1,
        )
        mix = jnp.dot(tmat[r], perturb, preferred_element_type=F32)
        for half in range(2):
            mixed[half, pl.ds(r, members, stride=RB), :] = mix[
                :, half * LANES : (half + 1) * LANES
            ]
    for half in range(2):
        value = mixed[half].reshape(members, RB, LANES) + averages[half][None]
        results[:, 2 * pair + half] = value.astype(BF16)


def kernel(
    members,
    levels,
    nrows,
    ncols,
    states,
    obs_pert,
    obs_innov,
    obs_cell,
    count,
    fields,
    tmat,
    pert,
    innov,
    cell,
    packed,
    groups,
    right,
    weighted,
    products,
    spread,
    mixed,
    obs_in,
    state_send,
    state_recv,
    obs_send,
    obs_recv,
):
    col = lax.axis_index("gx")
    row = lax.axis_index("gy")
    share = members // ncols
    chunks = TY // RB

    loads = [
        pltpu.make_async_copy(source, into, obs_in.at[i])
        for i, (source, into) in enumerate(
            ((obs_pert, pert), (obs_innov, innov), (obs_cell, cell))
        )
    ]
    for load in loads:
        load.start()

    barrier = pltpu.get_barrier_semaphore()

    def greet(coords):
        pl.semaphore_signal(barrier, inc=1, device_id=coords, device_id_type=MESH)

    for d in range(1, ncols):
        greet({"gx": lax.rem(col + d, ncols)})
    for a in (-1, 1):

        @pl.when(jnp.logical_and(row + a >= 0, row + a < nrows))
        def _():
            for b in (-1, 0, 1):
                greet({"gx": wrap(col + b, ncols), "gy": row + a})

    inner = jnp.logical_and(row > 0, row < nrows - 1)
    pl.semaphore_wait(barrier, ncols - 1 + jnp.where(inner, 6, 3))

    def obs_copy(slot, a, coords):
        return pltpu.make_async_remote_copy(
            src_ref=packed,
            dst_ref=groups.at[slot],
            send_sem=obs_send.at[slot],
            recv_sem=obs_recv.at[a + 1],
            device_id=coords,
            device_id_type=MESH,
        )

    def obs_plain(a, b, act):
        slot = (a + 1) * 3 + b + 1
        if a == 0 and b == 0:
            return

        def go():
            act(obs_copy(slot, a, {"gx": wrap(col - b, ncols), "gy": row - a}))

        if a == 0:
            go()
        else:
            pl.when(jnp.logical_and(row - a >= 0, row - a < nrows))(go)

    def obs_fold(b, act, act_local):
        slot = 6 + b + 1
        target = lax.rem(2 * ncols - 1 + b - col, ncols)
        at_fold = row == nrows - 1

        @pl.when(jnp.logical_and(at_fold, target != col))
        def _():
            act(
                pltpu.make_async_remote_copy(
                    src_ref=packed,
                    dst_ref=groups.at[slot],
                    send_sem=obs_send.at[9 + b + 1],
                    recv_sem=obs_recv.at[2],
                    device_id={"gx": target},
                    device_id_type=MESH,
                )
            )

        if act_local:

            @pl.when(jnp.logical_and(at_fold, target == col))
            def _():
                pltpu.make_async_copy(packed, groups.at[slot], obs_recv.at[2]).start()

    side = 4

    def distance(d):
        dy, dz = d // side, d % side
        return min(dy, side - dy) + min(dz, side - dz)

    order = sorted(range(1, ncols), key=distance)
    yy = col // side
    zz = lax.rem(col, side)
    odd = lax.rem(row, 2) == 1

    def states_of(target, c, some):
        return states.at[
            :, some, pl.ds(pl.multiple_of(c * RB, RB), RB), pl.ds(pl.multiple_of(target * TX, TX), TX)
        ]

    def issue(c, _):
        pltpu.make_async_copy(
            states_of(col, c, slice(None)), fields.at[c, pl.ds(col * share, share)], state_recv.at[c]
        ).start()
        for half in range(2):
            some = pl.ds(half * (levels // 2), levels // 2)
            for d in order:
                dy, dz = d // side, d % side
                dy = jnp.where(odd, side - dy, dy)
                dz = jnp.where(odd, side - dz, dz)
                target = lax.rem(yy + dy, side) * side + lax.rem(zz + dz, side)
                pltpu.make_async_remote_copy(
                    src_ref=states_of(target, c, some),
                    dst_ref=fields.at[c, pl.ds(col * share, share), some],
                    send_sem=state_send.at[c],
                    recv_sem=state_recv.at[c],
                    device_id={"gx": target},
                    device_id_type=MESH,
                ).start()
        return 0

    issue(0, 0)
    for load in loads:
        load.wait()
    filled = lax.broadcasted_iota(jnp.int32, (1, LANES), 1) < count[0, 0]
    packed[0:members] = jnp.where(filled, pert[...].astype(F32), 0.0).astype(BF16)
    cells = cell[...]
    packed[members:] = jnp.concatenate(
        [
            jnp.where(filled, innov[...].astype(F32), 0.0),
            lax.shift_right_logical(cells, 7).astype(F32),
            lax.bitwise_and(cells, 127).astype(F32),
            jnp.zeros((PK - members - 3, LANES), F32),
        ],
        axis=0,
    ).astype(BF16)
    issue(1, 0)
    for a in (0, 1, -1):
        for b in (-1, 0, 1):
            obs_plain(a, b, lambda copy: copy.start())
    for b in (-1, 0, 1):
        obs_fold(b, lambda copy: copy.start(), True)
    pltpu.make_async_copy(packed, groups.at[4], obs_recv.at[1]).start()

    lax.fori_loop(2, chunks, issue, 0)

    @pl.when(row == 0)
    def _():
        groups[0:3] = jnp.zeros((3, PK, LANES), BF16)

    @pl.when(row > 0)
    def _():
        three = groups.at[0:3]
        pltpu.make_async_copy(three, three, obs_recv.at[0]).wait()

    for a in (0, 1):
        three = groups.at[3 * (a + 1) : 3 * (a + 2)]
        pltpu.make_async_copy(three, three, obs_recv.at[a + 1]).wait()

    live = lax.broadcasted_iota(jnp.int32, (LANES, LANES), 0) < members
    for g in range(9):
        part = jnp.concatenate([groups[g], jnp.zeros((LANES - PK, LANES), BF16)], axis=0)
        right[:, g * LANES : (g + 1) * LANES] = jnp.where(
            live, part.astype(F32), 0.0
        ).astype(BF16)

    eye = (
        lax.broadcasted_iota(jnp.int32, (members, LANES), 0)
        == lax.broadcasted_iota(jnp.int32, (members, LANES), 1)
    ).astype(F32)
    width_x = float(TX * ncols)
    height_y = float(TY * nrows)

    def weigh(c):
        block_y = (
            row * TY + c * RB + lax.broadcasted_iota(jnp.int32, (RB, LANES), 0)
        ).astype(F32)
        for g in range(9):
            a, b = g // 3 - 1, g % 3 - 1
            around = groups[g].astype(F32)
            src_row = row + a
            src_col = wrap(col + b, ncols)
            local_row = around[members + 1 : members + 2]
            local_col = around[members + 2 : members + 3]
            if a == 1:
                folded = row == nrows - 1
                src_row = jnp.where(folded, nrows - 1, src_row)
                src_col = jnp.where(folded, wrap(ncols - 1 - col + b, ncols), src_col)
            obs_y = (src_row * TY).astype(F32) + local_row
            obs_x = (src_col * TX).astype(F32) + local_col
            if a == 1:
                turn = jnp.where(folded, 1.0, 0.0)
                obs_y = obs_y + turn * (2.0 * height_y - 1.0 - 2.0 * obs_y)
                obs_x = obs_x + turn * (width_x - 1.0 - 2.0 * obs_x)
            gap_y = obs_y - block_y
            offset = obs_x - (col * TX).astype(F32)
            offset = jnp.where(offset < 0.0, offset + width_x, offset)
            gap_x = jnp.where(
                offset < TX, 0.0, jnp.minimum(offset - (TX - 1.0), width_x - offset)
            )
            radius = float(TY // 2)
            scaled = jnp.minimum(1.0, (gap_x * gap_x + gap_y * gap_y) / (radius * radius))
            taper = (1.0 - scaled) * (1.0 - scaled)
            for r in range(RB):
                weighted[r * PK : (r + 1) * PK, g * LANES : (g + 1) * LANES] = (
                    around * taper[r : r + 1]
                ).astype(BF16)
        products[...] = lax.dot_general(
            weighted[...],
            right[...],
            (((1,), (1,)), ((), ())),
            preferred_element_type=F32,
        )

    def transforms(rows):
        scale, iterate, inverse = {}, {}, {}
        for r in rows:
            cov = products[r * PK : r * PK + members]
            system = eye + tall(cov).T[:members] * (1.0 / (members - 1.0))
            total = jnp.sum(jnp.sum(system * system, axis=0, keepdims=True), axis=1, keepdims=True)
            scale[r] = jnp.sqrt(total)
            iterate[r] = system / scale[r]
        for r in rows:
            inverse[r] = 1.5 * eye - 0.5 * iterate[r]
        iterate = {r: product(split(iterate[r]), split(inverse[r])) for r in rows}
        for sweep in range(1, NS_ITERS):
            inv = {r: split(inverse[r]) for r in rows}
            itr = {r: split(iterate[r]) for r in rows}
            both = {r: product(inv[r], itr[r]) for r in rows}
            cor = {r: split(1.5 * eye - 0.5 * both[r]) for r in rows}
            if sweep < NS_ITERS - 1:
                iterate = {r: product(itr[r], cor[r]) for r in rows}
            inverse = {r: product(cor[r], inv[r]) for r in rows}
        for r in rows:
            inv = split(inverse[r])
            projected = products[r * PK + members : r * PK + members + 8]
            once = product(split(projected), inv)
            mean = product(split(once), inv)[0:1]
            tmat[r] = (
                inverse[r] / jnp.sqrt(scale[r]) + mean / (scale[r] * (members - 1.0))
            ).astype(BF16)

    def step(c, _):
        weigh(c)
        for first in range(0, RB, 4):
            transforms(range(first, first + 4))
        pltpu.make_async_copy(fields.at[c], fields.at[c], state_recv.at[c]).wait()

        @pl.when(c < chunks - 1)
        def _():
            here = fields.at[c]
            for pair in range(levels // 2):
                analyse(members, here, tmat, spread, mixed, here, pair)

        return 0

    lax.fori_loop(0, chunks, step, 0)

    def sent(c, _):
        part = fields.at[c, 0 : (ncols - 1) * share]
        pltpu.make_async_copy(part, part, state_send.at[c]).wait()
        return 0

    lax.fori_loop(0, chunks, sent, 0)
    for a in (0, 1, -1):
        for b in (-1, 0, 1):
            obs_plain(a, b, lambda copy: copy.wait_send())
    for b in (-1, 0, 1):
        obs_fold(b, lambda copy: copy.wait_send(), False)


def place(members, levels, chunks, fields, tmat, out, spread, mixed, last, sem):
    copies = [
        pltpu.make_async_copy(fields.at[c], out.at[:, :, c * RB : (c + 1) * RB, :], sem.at[c])
        for c in range(chunks - 1)
    ]
    for copy in copies:
        copy.start()
    c = chunks - 1
    for pair in range(levels // 2):
        analyse(members, fields.at[c], tmat, spread, mixed, last, pair)
        some = slice(2 * pair, 2 * pair + 2)
        copies.append(
            pltpu.make_async_copy(
                last.at[:, some], out.at[:, some, c * RB : (c + 1) * RB, :], sem.at[c + pair]
            )
        )
        copies[-1].start()
    for copy in copies:
        copy.wait()


def body(states, obs_pert, obs_innov, obs_cell, obs_count):
    members = obs_pert.shape[0]
    slots = obs_pert.shape[2]
    levels = states.shape[1]
    ncols = lax.axis_size("gx")
    nrows = lax.axis_size("gy")
    chunks = TY // RB
    hbm = pl.BlockSpec(memory_space=pltpu.HBM)
    vmem = pl.BlockSpec(memory_space=pltpu.VMEM)
    work = [
        pltpu.VMEM((2, members * RB, LANES), F32),
        pltpu.VMEM((2, members * RB, LANES), F32),
    ]
    fields, tmat = pl.pallas_call(
        functools.partial(kernel, members, levels, nrows, ncols),
        out_shape=(
            jax.ShapeDtypeStruct((chunks, members, levels, RB, TX), BF16),
            jax.ShapeDtypeStruct((RB, members, LANES), BF16),
        ),
        in_specs=[hbm] * 4 + [pl.BlockSpec(memory_space=pltpu.SMEM)],
        out_specs=(vmem, vmem),
        scratch_shapes=[
            pltpu.VMEM((members, slots), BF16),
            pltpu.VMEM((1, slots), BF16),
            pltpu.VMEM((1, slots), jnp.int32),
            pltpu.VMEM((PK, LANES), BF16),
            pltpu.VMEM((9, PK, LANES), BF16),
            pltpu.VMEM((LANES, 9 * LANES), BF16),
            pltpu.VMEM((RB * PK, 9 * LANES), BF16),
            pltpu.VMEM((RB * PK, LANES), F32),
            *work,
            pltpu.SemaphoreType.DMA((3,)),
            pltpu.SemaphoreType.DMA((chunks,)),
            pltpu.SemaphoreType.DMA((chunks,)),
            pltpu.SemaphoreType.DMA((12,)),
            pltpu.SemaphoreType.DMA((3,)),
        ],
        compiler_params=pltpu.CompilerParams(
            collective_id=0, has_side_effects=True, vmem_limit_bytes=40 << 20
        ),
        name="exchange",
    )(
        states,
        *(
            pltpu.with_memory_space_constraint(value, pltpu.HBM)
            for value in (obs_pert.reshape(members, slots), obs_innov, obs_cell)
        ),
        obs_count,
    )
    return pl.pallas_call(
        functools.partial(place, members, levels, chunks),
        out_shape=jax.ShapeDtypeStruct((members, levels, TY, TX), BF16),
        in_specs=[vmem, vmem],
        out_specs=hbm,
        scratch_shapes=[
            *work,
            pltpu.VMEM((members, levels, RB, TX), BF16),
            pltpu.SemaphoreType.DMA((chunks - 1 + levels // 2,)),
        ],
        compiler_params=pltpu.CompilerParams(vmem_limit_bytes=24 << 20),
        name="place",
    )(fields, tmat)


def solution(mesh):
    return jax.shard_map(
        body,
        mesh=mesh,
        in_specs=(
            P("gx", None, "gy", None),
            P(None, "gy", "gx"),
            P("gy", "gx"),
            P("gy", "gx"),
            P("gy", "gx"),
        ),
        out_specs=P(None, None, "gy", "gx"),
        check_vma=False,
    )
```

```python
import functools

import jax
import jax.numpy as jnp
from jax import lax
from jax.experimental import pallas as pl
from jax.experimental.pallas import tpu as pltpu
from jax.sharding import PartitionSpec as P

MESH = pl.DeviceIdType.MESH
F32 = jnp.float32
BF16 = jnp.bfloat16

TX = 128
TY = 64
NS_ITERS = 4
RB = 8
PK = 96
LANES = 128


def wrap(value, count):
    return lax.rem(value + count, count)


def split(value):
    high = value.astype(BF16)
    low = (value - high.astype(F32)).astype(BF16)
    return high, low


def tall(value):
    rows = value.shape[0]
    return jnp.concatenate([value, jnp.zeros((LANES - rows, value.shape[1]), value.dtype)], axis=0)


def product(left, right):
    lh, ll = left
    rh, rl = (tall(part) for part in right)
    lhs = jnp.concatenate([lh, ll], axis=1)
    rhs = jnp.concatenate(
        [
            jnp.concatenate([rh, rl], axis=1),
            jnp.concatenate([rh, jnp.zeros_like(rl)], axis=1),
        ],
        axis=0,
    )
    both = jnp.dot(lhs, rhs, preferred_element_type=F32)
    return both[:, :LANES] + both[:, LANES:]


def analyse(members, fields, tmat, spread, mixed, results, pair):
    averages = []
    for half in range(2):
        field = fields[:, 2 * pair + half].astype(F32)
        average = jnp.sum(field, axis=0) * (1.0 / members)
        averages.append(average)
        spread[half] = (field - average[None]).reshape(members * RB, LANES)
    for r in range(RB):
        perturb = jnp.concatenate(
            [
                tall(spread[half, pl.ds(r, members, stride=RB), :].astype(BF16))
                for half in range(2)
            ],
            axis=1,
        )
        mix = jnp.dot(tmat[r], perturb, preferred_element_type=F32)
        for half in range(2):
            mixed[half, pl.ds(r, members, stride=RB), :] = mix[
                :, half * LANES : (half + 1) * LANES
            ]
    for half in range(2):
        value = mixed[half].reshape(members, RB, LANES) + averages[half][None]
        results[:, 2 * pair + half] = value.astype(BF16)


def kernel(
    members,
    levels,
    nrows,
    ncols,
    states,
    obs_pert,
    obs_innov,
    obs_cell,
    count,
    fields,
    tmat,
    pert,
    innov,
    cell,
    packed,
    groups,
    right,
    weighted,
    products,
    spread,
    mixed,
    obs_in,
    state_send,
    state_recv,
    obs_send,
    obs_recv,
):
    col = lax.axis_index("gx")
    row = lax.axis_index("gy")
    share = members // ncols
    chunks = TY // RB

    loads = [
        pltpu.make_async_copy(source, into, obs_in.at[i])
        for i, (source, into) in enumerate(
            ((obs_pert, pert), (obs_innov, innov), (obs_cell, cell))
        )
    ]

    barrier = pltpu.get_barrier_semaphore()

    def greet(coords):
        pl.semaphore_signal(barrier, inc=1, device_id=coords, device_id_type=MESH)

    for d in range(1, ncols):
        greet({"gx": lax.rem(col + d, ncols)})
    for a in (-1, 1):

        @pl.when(jnp.logical_and(row + a >= 0, row + a < nrows))
        def _():
            for b in (-1, 0, 1):
                greet({"gx": wrap(col + b, ncols), "gy": row + a})

    for load in loads:
        load.start()
    inner = jnp.logical_and(row > 0, row < nrows - 1)
    pl.semaphore_wait(barrier, ncols - 1 + jnp.where(inner, 6, 3))

    def obs_copy(slot, a, coords):
        return pltpu.make_async_remote_copy(
            src_ref=packed,
            dst_ref=groups.at[slot],
            send_sem=obs_send.at[slot],
            recv_sem=obs_recv.at[a + 1],
            device_id=coords,
            device_id_type=MESH,
        )

    def obs_plain(a, b, act):
        slot = (a + 1) * 3 + b + 1
        if a == 0 and b == 0:
            return

        def go():
            act(obs_copy(slot, a, {"gx": wrap(col - b, ncols), "gy": row - a}))

        if a == 0:
            go()
        else:
            pl.when(jnp.logical_and(row - a >= 0, row - a < nrows))(go)

    def obs_fold(b, act, act_local):
        slot = 6 + b + 1
        target = lax.rem(2 * ncols - 1 + b - col, ncols)
        at_fold = row == nrows - 1

        @pl.when(jnp.logical_and(at_fold, target != col))
        def _():
            act(
                pltpu.make_async_remote_copy(
                    src_ref=packed,
                    dst_ref=groups.at[slot],
                    send_sem=obs_send.at[9 + b + 1],
                    recv_sem=obs_recv.at[2],
                    device_id={"gx": target},
                    device_id_type=MESH,
                )
            )

        if act_local:

            @pl.when(jnp.logical_and(at_fold, target == col))
            def _():
                pltpu.make_async_copy(packed, groups.at[slot], obs_recv.at[2]).start()

    side = 4

    def distance(d):
        dy, dz = d // side, d % side
        return min(dy, side - dy) + min(dz, side - dz)

    order = sorted(range(1, ncols), key=distance)
    yy = col // side
    zz = lax.rem(col, side)
    odd = lax.rem(row, 2) == 1

    def states_of(target, c, some):
        return states.at[
            :, some, pl.ds(pl.multiple_of(c * RB, RB), RB), pl.ds(pl.multiple_of(target * TX, TX), TX)
        ]

    def issue(c, _):
        pltpu.make_async_copy(
            states_of(col, c, slice(None)), fields.at[c, pl.ds(col * share, share)], state_recv.at[c]
        ).start()
        for half in range(2):
            some = pl.ds(half * (levels // 2), levels // 2)
            for d in order:
                dy, dz = d // side, d % side
                dy = jnp.where(odd, side - dy, dy)
                dz = jnp.where(odd, side - dz, dz)
                target = lax.rem(yy + dy, side) * side + lax.rem(zz + dz, side)
                pltpu.make_async_remote_copy(
                    src_ref=states_of(target, c, some),
                    dst_ref=fields.at[c, pl.ds(col * share, share), some],
                    send_sem=state_send.at[c],
                    recv_sem=state_recv.at[c],
                    device_id={"gx": target},
                    device_id_type=MESH,
                ).start()
        return 0

    issue(0, 0)
    for load in loads:
        load.wait()
    filled = lax.broadcasted_iota(jnp.int32, (1, LANES), 1) < count[0, 0]
    packed[0:members] = jnp.where(filled, pert[...].astype(F32), 0.0).astype(BF16)
    cells = cell[...]
    packed[members:] = jnp.concatenate(
        [
            jnp.where(filled, innov[...].astype(F32), 0.0),
            lax.shift_right_logical(cells, 7).astype(F32),
            lax.bitwise_and(cells, 127).astype(F32),
            jnp.zeros((PK - members - 3, LANES), F32),
        ],
        axis=0,
    ).astype(BF16)
    issue(1, 0)
    for a in (0, 1, -1):
        for b in (-1, 0, 1):
            obs_plain(a, b, lambda copy: copy.start())
    for b in (-1, 0, 1):
        obs_fold(b, lambda copy: copy.start(), True)
    pltpu.make_async_copy(packed, groups.at[4], obs_recv.at[1]).start()

    lax.fori_loop(2, chunks, issue, 0)

    @pl.when(row == 0)
    def _():
        groups[0:3] = jnp.zeros((3, PK, LANES), BF16)

    @pl.when(row > 0)
    def _():
        three = groups.at[0:3]
        pltpu.make_async_copy(three, three, obs_recv.at[0]).wait()

    for a in (0, 1):
        three = groups.at[3 * (a + 1) : 3 * (a + 2)]
        pltpu.make_async_copy(three, three, obs_recv.at[a + 1]).wait()

    live = lax.broadcasted_iota(jnp.int32, (LANES, LANES), 0) < members
    for g in range(9):
        part = jnp.concatenate([groups[g], jnp.zeros((LANES - PK, LANES), BF16)], axis=0)
        right[:, g * LANES : (g + 1) * LANES] = jnp.where(
            live, part.astype(F32), 0.0
        ).astype(BF16)

    eye = (
        lax.broadcasted_iota(jnp.int32, (members, LANES), 0)
        == lax.broadcasted_iota(jnp.int32, (members, LANES), 1)
    ).astype(F32)
    width_x = float(TX * ncols)
    height_y = float(TY * nrows)

    def weigh(c):
        block_y = (
            row * TY + c * RB + lax.broadcasted_iota(jnp.int32, (RB, LANES), 0)
        ).astype(F32)
        for g in range(9):
            a, b = g // 3 - 1, g % 3 - 1
            around = groups[g].astype(F32)
            src_row = row + a
            src_col = wrap(col + b, ncols)
            local_row = around[members + 1 : members + 2]
            local_col = around[members + 2 : members + 3]
            if a == 1:
                folded = row == nrows - 1
                src_row = jnp.where(folded, nrows - 1, src_row)
                src_col = jnp.where(folded, wrap(ncols - 1 - col + b, ncols), src_col)
            obs_y = (src_row * TY).astype(F32) + local_row
            obs_x = (src_col * TX).astype(F32) + local_col
            if a == 1:
                turn = jnp.where(folded, 1.0, 0.0)
                obs_y = obs_y + turn * (2.0 * height_y - 1.0 - 2.0 * obs_y)
                obs_x = obs_x + turn * (width_x - 1.0 - 2.0 * obs_x)
            gap_y = obs_y - block_y
            offset = obs_x - (col * TX).astype(F32)
            offset = jnp.where(offset < 0.0, offset + width_x, offset)
            gap_x = jnp.where(
                offset < TX, 0.0, jnp.minimum(offset - (TX - 1.0), width_x - offset)
            )
            radius = float(TY // 2)
            scaled = jnp.minimum(1.0, (gap_x * gap_x + gap_y * gap_y) / (radius * radius))
            taper = (1.0 - scaled) * (1.0 - scaled)
            for r in range(RB):
                weighted[r * PK : (r + 1) * PK, g * LANES : (g + 1) * LANES] = (
                    around * taper[r : r + 1]
                ).astype(BF16)
        products[...] = lax.dot_general(
            weighted[...],
            right[...],
            (((1,), (1,)), ((), ())),
            preferred_element_type=F32,
        )

    def transforms(rows):
        scale, iterate, inverse = {}, {}, {}
        for r in rows:
            cov = products[r * PK : r * PK + members]
            system = eye + tall(cov).T[:members] * (1.0 / (members - 1.0))
            total = jnp.sum(jnp.sum(system * system, axis=0, keepdims=True), axis=1, keepdims=True)
            scale[r] = jnp.sqrt(total)
            iterate[r] = system / scale[r]
        for r in rows:
            inverse[r] = 1.5 * eye - 0.5 * iterate[r]
        iterate = {r: product(split(iterate[r]), split(inverse[r])) for r in rows}
        for sweep in range(1, NS_ITERS):
            inv = {r: split(inverse[r]) for r in rows}
            itr = {r: split(iterate[r]) for r in rows}
            both = {r: product(inv[r], itr[r]) for r in rows}
            cor = {r: split(1.5 * eye - 0.5 * both[r]) for r in rows}
            if sweep < NS_ITERS - 1:
                iterate = {r: product(itr[r], cor[r]) for r in rows}
            inverse = {r: product(cor[r], inv[r]) for r in rows}
        for r in rows:
            inv = split(inverse[r])
            projected = products[r * PK + members : r * PK + members + 8]
            once = product(split(projected), inv)
            mean = product(split(once), inv)[0:1]
            tmat[r] = (
                inverse[r] / jnp.sqrt(scale[r]) + mean / (scale[r] * (members - 1.0))
            ).astype(BF16)

    def step(c, _):
        weigh(c)
        for first in range(0, RB, 4):
            transforms(range(first, first + 4))
        pltpu.make_async_copy(fields.at[c], fields.at[c], state_recv.at[c]).wait()

        @pl.when(c < chunks - 1)
        def _():
            here = fields.at[c]
            for pair in range(levels // 2):
                analyse(members, here, tmat, spread, mixed, here, pair)

        return 0

    lax.fori_loop(0, chunks, step, 0)

    def sent(c, _):
        part = fields.at[c, 0 : (ncols - 1) * share]
        pltpu.make_async_copy(part, part, state_send.at[c]).wait()
        return 0

    lax.fori_loop(0, chunks, sent, 0)
    for a in (0, 1, -1):
        for b in (-1, 0, 1):
            obs_plain(a, b, lambda copy: copy.wait_send())
    for b in (-1, 0, 1):
        obs_fold(b, lambda copy: copy.wait_send(), False)


def place(members, levels, chunks, fields, tmat, out, spread, mixed, last, sem):
    copies = [
        pltpu.make_async_copy(fields.at[c], out.at[:, :, c * RB : (c + 1) * RB, :], sem.at[c])
        for c in range(chunks - 1)
    ]
    for copy in copies:
        copy.start()
    c = chunks - 1
    for pair in range(levels // 2):
        analyse(members, fields.at[c], tmat, spread, mixed, last, pair)
        some = slice(2 * pair, 2 * pair + 2)
        copies.append(
            pltpu.make_async_copy(
                last.at[:, some], out.at[:, some, c * RB : (c + 1) * RB, :], sem.at[c + pair]
            )
        )
        copies[-1].start()
    for copy in copies:
        copy.wait()


def body(states, obs_pert, obs_innov, obs_cell, obs_count):
    members = obs_pert.shape[0]
    slots = obs_pert.shape[2]
    levels = states.shape[1]
    ncols = lax.axis_size("gx")
    nrows = lax.axis_size("gy")
    chunks = TY // RB
    hbm = pl.BlockSpec(memory_space=pltpu.HBM)
    vmem = pl.BlockSpec(memory_space=pltpu.VMEM)
    work = [
        pltpu.VMEM((2, members * RB, LANES), F32),
        pltpu.VMEM((2, members * RB, LANES), F32),
    ]
    fields, tmat = pl.pallas_call(
        functools.partial(kernel, members, levels, nrows, ncols),
        out_shape=(
            jax.ShapeDtypeStruct((chunks, members, levels, RB, TX), BF16),
            jax.ShapeDtypeStruct((RB, members, LANES), BF16),
        ),
        in_specs=[hbm] * 4 + [pl.BlockSpec(memory_space=pltpu.SMEM)],
        out_specs=(vmem, vmem),
        scratch_shapes=[
            pltpu.VMEM((members, slots), BF16),
            pltpu.VMEM((1, slots), BF16),
            pltpu.VMEM((1, slots), jnp.int32),
            pltpu.VMEM((PK, LANES), BF16),
            pltpu.VMEM((9, PK, LANES), BF16),
            pltpu.VMEM((LANES, 9 * LANES), BF16),
            pltpu.VMEM((RB * PK, 9 * LANES), BF16),
            pltpu.VMEM((RB * PK, LANES), F32),
            *work,
            pltpu.SemaphoreType.DMA((3,)),
            pltpu.SemaphoreType.DMA((chunks,)),
            pltpu.SemaphoreType.DMA((chunks,)),
            pltpu.SemaphoreType.DMA((12,)),
            pltpu.SemaphoreType.DMA((3,)),
        ],
        compiler_params=pltpu.CompilerParams(
            collective_id=0, has_side_effects=True, vmem_limit_bytes=40 << 20
        ),
        name="exchange",
    )(
        states,
        *(
            pltpu.with_memory_space_constraint(value, pltpu.HBM)
            for value in (obs_pert.reshape(members, slots), obs_innov, obs_cell)
        ),
        obs_count,
    )
    return pl.pallas_call(
        functools.partial(place, members, levels, chunks),
        out_shape=jax.ShapeDtypeStruct((members, levels, TY, TX), BF16),
        in_specs=[vmem, vmem],
        out_specs=hbm,
        scratch_shapes=[
            *work,
            pltpu.VMEM((members, levels, RB, TX), BF16),
            pltpu.SemaphoreType.DMA((chunks - 1 + levels // 2,)),
        ],
        compiler_params=pltpu.CompilerParams(vmem_limit_bytes=24 << 20),
        name="place",
    )(fields, tmat)


def solution(mesh):
    return jax.shard_map(
        body,
        mesh=mesh,
        in_specs=(
            P("gx", None, "gy", None),
            P(None, "gy", "gx"),
            P("gy", "gx"),
            P("gy", "gx"),
            P("gy", "gx"),
        ),
        out_specs=P(None, None, "gy", "gx"),
        check_vma=False,
    )
```
